256 devices in a mesh: unit: 4 (over y_lo, core), zero: 32 (over z, y_hi, x_hi), cols: 2 (over x_lo).
Axes of the slice: x: 4 (x_hi: 2, x_lo: 2; x = x_hi * 2 + x_lo), y: 4 (y_hi: 2, y_lo: 2; y = y_hi * 2 + y_lo), z: 8, core: 2. Of those that a mesh axis runs over, the one named last changes fastest.
Arguments:
- weight_gate: bfloat16 [20480, 13824], P(('unit', 'zero'), 'cols'), parts along dimension 0, may hold values from -0.15625 to 0.15625
- low_gate: bfloat16 [20480, 32], P(('unit', 'zero')), parts along dimension 0, may hold values from -0.078125 to 0.078125
- high_gate: bfloat16 [128, 13824], P('unit', 'cols'), parts along dimension 0, may hold values from -1 to 1
- weight_up: bfloat16 [20480, 13824], P(('unit', 'zero'), 'cols'), parts along dimension 0, may hold values from -0.15625 to 0.15625
- low_up: bfloat16 [20480, 32], P(('unit', 'zero')), parts along dimension 0, may hold values from -0.078125 to 0.078125
- high_up: bfloat16 [128, 13824], P('unit', 'cols'), parts along dimension 0, may hold values from -1 to 1
- norm_train: float32 [20480], P(('unit', 'zero', 'cols')), parts along dimension 0, may hold values from 0.25 to 1.75
- norm_step: float32 [20480], P(('unit', 'zero', 'cols')), parts along dimension 0, may hold values from -0.3 to 0.3
Outputs:
- final_gate: bfloat16 [20480, 13824], P('unit', ('cols', 'zero')), parts along dimension 0
- final_up: bfloat16 [20480, 13824], P('unit', ('cols', 'zero')), parts along dimension 0
- scale_gate: float32 [55296], P(('unit', 'cols', 'zero')), parts along dimension 0
- scale_up: float32 [55296], P(('unit', 'cols', 'zero')), parts along dimension 0
- serve_norm: bfloat16 [20480], P('unit'), parts along dimension 0
The draws below stay inside these ranges and needn't reach their ends.
There are 4 independent parts, one for each index of `unit`. The reference program is written for one: setup_inputs(seed, part) draws one part's arguments, and reference() takes and returns one part's arrays. A program takes and returns all parts, laid end to end along the dimension named above; each array names one. Nothing has to cross between parts.
All inputs are finite; a program needn't handle non-finite values. Where the reference program divides by a largest or mean magnitude, that divisor is 1e-20 or more.
Results may differ from the reference program's by a relative error of at most 0.001.
Values may be sent and summed in bfloat16 or wider, within the bound.
No kernel may reach another device: no remote copies, remote signals or barrier semaphores. Data moves between devices by JAX's collectives and lax.ppermute only.
A program may use at most 128 MiB of HBM per device.

```python
import jax
import jax.numpy as jnp

D_MODEL = 5120
D_INNER = 13824
RANK = 32


def strengthened(entries, own_key, source, target, parts, factor):
    def block_of(position):
        return (jnp.arange(entries.shape[position]) // (entries.shape[position] // parts)).reshape((-1,) + (1,) * (entries.ndim - 1 - position))

    one_side = jax.random.permutation(own_key, parts)[block_of(target)]
    other_side = (block_of(target) + parts // 2) % parts
    return jnp.where((block_of(source) == one_side) | (block_of(source) == other_side), factor * entries, entries)


def levels(own_key, extent, split, least, top_value):
    level, own = 1.0, jax.random.fold_in(own_key, 6)
    for dim, blocks in split:
        draws = jnp.exp(jax.random.uniform(jax.random.fold_in(own, dim), (blocks,), jnp.float32, least / len(split), top_value / len(split)))
        level = level * jnp.repeat(draws, extent[dim] // blocks).reshape([-1 if axis == dim else 1 for axis in range(len(extent))])
    return level


def normal_values(rng, extent, deviation, most, cuts=(), kind=jnp.bfloat16):
    level = levels(rng, extent, cuts, -0.22, 0.18) if cuts else 1.0
    entries = jax.random.normal(rng, extent, jnp.float32) * deviation * level
    return jnp.minimum(jnp.maximum(entries, -most), most).astype(kind)


def gaussian_with(stream_key, extent, width, bound, shards, heavy, held_as=jnp.bfloat16):
    values = width * jax.random.normal(stream_key, extent, jnp.float32)
    if shards:
        values = values * levels(stream_key, extent, shards, -0.22, 0.18)
    return jnp.clip(strengthened(values, jax.random.fold_in(stream_key, 3), *heavy), -bound, bound).astype(held_as)


def setup_inputs(seed: int = 0, part: int = 0) -> dict:
    keys = jax.random.split(jax.random.key(seed), 9)
    part_splits = jax.random.split(jax.random.fold_in(keys[8], part), 9)
    return {
        "weight_gate": gaussian_with(part_splits[0], (D_MODEL, D_INNER), D_MODEL ** -0.5, 0.15625, ((0, 32), (1, 2)), (0, 1, 32, 2.75)),
        "low_gate": normal_values(part_splits[1], (D_MODEL, RANK), D_MODEL ** -0.5, 0.078125, ((0, 32),)),
        "high_gate": normal_values(part_splits[2], (RANK, D_INNER), RANK ** -0.5, 1.0, ((1, 2),)),
        "weight_up": gaussian_with(part_splits[3], (D_MODEL, D_INNER), D_MODEL ** -0.5, 0.15625, ((0, 32), (1, 2)), (0, 1, 32, 2.75)),
        "low_up": normal_values(part_splits[4], (D_MODEL, RANK), D_MODEL ** -0.5, 0.078125, ((0, 32),)),
        "high_up": normal_values(part_splits[5], (RANK, D_INNER), RANK ** -0.5, 1.0, ((1, 2),)),
        "norm_train": jnp.clip(1.0 + 0.15 * jax.random.normal(part_splits[6], (D_MODEL,), jnp.float32), 0.25, 1.75),
        "norm_step": jnp.clip(jax.random.uniform(part_splits[7], (D_MODEL,), jnp.float32, -0.3, 0.3) * levels(part_splits[7], (D_MODEL,), ((0, 64),), -0.4, 0.0), -0.3, 0.3),
    }


mix_rate = 0.5


def reference(weight_gate, low_gate, high_gate, weight_up, low_up, high_up, norm_train, norm_step):
    result_gate = weight_gate.astype(jnp.float32) + mix_rate * jnp.dot(low_gate, high_gate, preferred_element_type=jnp.float32)
    result_up = weight_up.astype(jnp.float32) + mix_rate * jnp.dot(low_up, high_up, preferred_element_type=jnp.float32)
    scale_gate = jnp.sum(jnp.abs(result_gate), axis=0) / D_MODEL
    final_gate = (result_gate / scale_gate).astype(jnp.bfloat16)
    scale_up = jnp.sum(jnp.abs(result_up), axis=0) / D_MODEL
    final_up = (result_up / scale_up).astype(jnp.bfloat16)
    serve_norm = (norm_train + norm_step).astype(jnp.bfloat16)
    return final_gate, final_up, scale_gate, scale_up, serve_norm
```

```python
import jax
import jax.numpy as jnp
from jax import lax
from jax.experimental import pallas as pl
from jax.experimental.pallas import tpu as pltpu
from jax.sharding import PartitionSpec as P

D_MODEL = 5120
MIX = 0.5
NZ = 8
NQ = 4
ROWS = 160
COLS = 216
RANK = 32
SPAN = NQ * COLS
TILES = 7
EXTRA = 48
BLOCK = TILES * ROWS + EXTRA
PART = 2 * ROWS + EXTRA
LAST = 51

Z_GROUPS = [[z * NQ + q for z in range(NZ)] for q in range(NQ)]
bf16, f32 = jnp.bfloat16, jnp.float32


def lanes(shape):
    return lax.broadcasted_iota(jnp.int32, shape, len(shape) - 1)


def rows(shape):
    return lax.broadcasted_iota(jnp.int32, shape, len(shape) - 2)


def place_t(low_t, period, first):
    shape = (RANK, 128)
    hit = (lanes(shape) >= first) & ((lanes(shape) - first) % period == rows(shape))
    return lax.dot_general(
        low_t, hit.astype(bf16), (((0,), (0,)), ((), ())), preferred_element_type=f32
    )


def pack_gate(weight, low_gate, low_up, train, step, out):
    wide = (ROWS, 128)
    low_g = place_t(low_gate[...], 128, 96)
    low_u = place_t(low_up[...], 32, 0)
    group = lanes((40, 128)) // 32
    packed = jnp.zeros((40, 128), f32)
    for g in range(4):
        packed = jnp.where(group == g, low_u[40 * g : 40 * g + 40], packed)
    norm = jnp.concatenate([train[...] + step[...], jnp.zeros((1, 48), f32)], axis=1)
    norm = jnp.broadcast_to(norm, (8, 128))
    extra = jnp.concatenate([packed, norm], axis=0).astype(bf16)
    for z in range(NZ):
        first, off = divmod(SPAN * z, 128)
        for j in range(TILES):
            t = first + j
            x = weight[:, 128 * t : 128 * t + 128].astype(f32)
            if off:
                x = pltpu.roll(x, 128 - off, 1)
                if j < TILES - 1 or off > 32:
                    y = weight[:, 128 * t + 128 : 128 * t + 256].astype(f32)
                    x = jnp.where(lanes(wide) < 128 - off, x, pltpu.roll(y, 128 - off, 1))
            if j == TILES - 1:
                x = jnp.where(lanes(wide) < 96, x, low_g)
            out[z, ROWS * j : ROWS * j + ROWS, :] = x.astype(bf16)
        out[z, ROWS * TILES : BLOCK, :] = extra


def window(x, off):
    return pltpu.roll(x, (384 - off) % 384, 1)[:, :256]


def pack_up(weight, high_gate, high_up, *outs):
    parts, mix, high = outs[:NQ], outs[NQ], outs[NQ + 1]
    place = lax.axis_index("zero")
    q = place % NQ
    for p in range(NQ):
        for z in range(NZ):
            start = COLS * (z * NQ + jnp.bitwise_xor(q, p))
            tile = jnp.minimum(start // 128, LAST)
            x = weight[:, pl.ds(pl.multiple_of(tile * 128, 128), 384)].astype(f32)
            x = window(x, start - 128 * tile).astype(bf16)
            parts[p][z, 0:ROWS, :] = x[:, :128]
            parts[p][z, ROWS : 2 * ROWS, :] = x[:, 128:]
    start = COLS * place
    tile = jnp.minimum(start // 128, LAST)
    at = pl.multiple_of(tile * 128, 128)

    def own(ref):
        x = pltpu.roll(ref[:, pl.ds(at, 384)].astype(f32), (384 - (start - 128 * tile)) % 384, 1)
        return x[:, :256].astype(bf16)

    def turned(h, first, width):
        shape = (RANK, width)
        hit = jnp.where(lanes(shape) == rows(shape) + first, MIX, 0.0).astype(bf16)
        return lax.dot_general(h, hit, (((0,), (0,)), ((), ())), preferred_element_type=f32)

    eye = (lanes((256, 256)) == rows((256, 256))) & (rows((256, 256)) < COLS)
    mix[...] = (eye.astype(f32) + turned(own(high_gate), COLS, 256)).astype(bf16)
    high[...] = turned(own(high_up), 0, 128).astype(bf16)


def turn_up(*refs):
    parts, out, x = refs[:NQ], refs[NQ], refs[NQ + 1]
    q = lax.axis_index("zero") % NQ
    eye = (lanes((COLS, 256)) == rows((COLS, 256))).astype(bf16)
    for z in range(NZ):
        for p in range(NQ):
            at = pl.multiple_of(jnp.bitwise_xor(q, p) * ROWS, ROWS)
            x[z % 2, pl.ds(at, ROWS), 0:128] = parts[p][z, 0:ROWS, :]
            x[z % 2, pl.ds(at, ROWS), 128:256] = parts[p][z, ROWS : 2 * ROWS, :]
        out[z] = lax.dot_general(
            eye, x[z % 2], (((1,), (1,)), ((), ())), preferred_element_type=f32
        ).astype(bf16)


def split_gate(block, *parts):
    q = lax.axis_index("zero") % NQ
    wide = (ROWS, 128)
    for z in range(NZ):
        low = pltpu.roll(block[z, ROWS * 6 : ROWS * 7, :].astype(f32), 120, 1)
        for p in range(NQ):
            start = COLS * jnp.bitwise_xor(q, p)
            tile = jnp.minimum(start // 128, TILES - 3)
            x = jnp.concatenate(
                [
                    block[z, pl.ds(pl.multiple_of((tile + k) * ROWS, ROWS), ROWS), :].astype(f32)
                    for k in range(3)
                ],
                axis=1,
            )
            x = window(x, start - 128 * tile)
            last = jnp.where(lanes(wide) < 88, x[:, 128:], jnp.where(lanes(wide) < 120, low, 0.0))
            parts[p][z, 0:ROWS, :] = x[:, :128].astype(bf16)
            parts[p][z, ROWS : 2 * ROWS, :] = last.astype(bf16)
            parts[p][z, 2 * ROWS : PART, :] = block[z, ROWS * TILES : BLOCK, :]


def scales(total):
    column = jnp.sum(total, axis=1, keepdims=True) / D_MODEL
    padded = jnp.concatenate([total, jnp.zeros((256 - COLS, 128), f32)], axis=0)
    row = jnp.sum(jnp.transpose(padded), axis=0, keepdims=True) / D_MODEL
    return column, row[:, :COLS]


def magnitudes(r):
    a = jnp.abs(r)
    return sum(a[:, 128 * k : 128 * k + 128] for k in range(5))


def last_gate(*refs):
    parts, mix = refs[:NQ], refs[NQ]
    out, scale, low, norm = refs[NQ + 1 : NQ + 5]
    x, lows, sums = refs[NQ + 5 :]
    q = lax.axis_index("zero") % NQ
    total = jnp.zeros((COLS, 128), f32)
    m = mix[0:COLS, :]
    pick = (lanes((RANK, 128)) == rows((RANK, 128))).astype(bf16)
    for z in range(NZ):
        for p in range(NQ):
            at = pl.multiple_of(jnp.bitwise_xor(q, p) * ROWS, ROWS)
            x[z % 2, pl.ds(at, ROWS), 0:128] = parts[p][z, 0:ROWS, :]
            x[z % 2, pl.ds(at, ROWS), 128:256] = parts[p][z, ROWS : 2 * ROWS, :]
            extra = parts[p][z, 2 * ROWS : PART, :].astype(f32)
            wide = jnp.concatenate(
                [pltpu.roll(extra[0:40], (128 - 32 * g) % 128, 1) for g in range(4)], axis=0
            )
            lows[z % 2, pl.ds(at, ROWS), :] = wide.astype(bf16)
            norm[z, pl.ds(jnp.bitwise_xor(q, p), 1), :] = extra[40:41]
        r = lax.dot_general(m, x[z % 2], (((1,), (1,)), ((), ())), preferred_element_type=f32)
        sums[:, 640 * z : 640 * z + 640] = r
        total = total + magnitudes(r)
        low[:, 640 * z : 640 * z + 640] = lax.dot_general(
            pick, lows[z % 2], (((1,), (1,)), ((), ())), preferred_element_type=f32
        ).astype(bf16)
    column, row = scales(total)
    scale[...] = row
    out[...] = (sums[...] * (1.0 / column)).astype(bf16)


def last_up(block, high, low, out, scale, sums):
    total = jnp.zeros((COLS, 128), f32)
    h = high[0:COLS, 0:RANK]
    for z in range(NZ):
        r = block[z].astype(f32) + jnp.dot(
            h, low[:, 640 * z : 640 * z + 640], preferred_element_type=f32
        )
        sums[:, 640 * z : 640 * z + 640] = r
        total = total + magnitudes(r)
    column, row = scales(total)
    scale[...] = row
    out[...] = (sums[...] * (1.0 / column)).astype(bf16)


def kernel(body, outs, scratch=()):
    return pl.pallas_call(
        body,
        out_shape=[jax.ShapeDtypeStruct(*o) for o in outs],
        scratch_shapes=list(scratch),
        compiler_params=pltpu.CompilerParams(vmem_limit_bytes=48 * 2**20),
    )


def along_z(x):
    flat = x.reshape(-1, x.shape[-1])
    return lax.all_to_all(
        flat, "zero", 0, 0, axis_index_groups=Z_GROUPS, tiled=True
    ).reshape(x.shape)


def across(parts):
    moved = [
        lax.ppermute(part, "zero", [(s, s ^ p) for s in range(NZ * NQ)])
        for p, part in enumerate(parts)
        if p
    ]
    return [parts[0], *moved]


def local(weight_gate, low_gate, high_gate, weight_up, low_up, high_up, norm_train, norm_step):
    (block,) = kernel(pack_gate, [((NZ, BLOCK, 128), bf16)])(
        weight_gate, low_gate.T, low_up.T, norm_train[None], norm_step[None]
    )
    block_in = along_z(block)
    *up_parts, mix, high = kernel(
        pack_up, [((NZ, 2 * ROWS, 128), bf16)] * NQ + [((256, 256), bf16), ((256, 128), bf16)]
    )(weight_up, high_gate, high_up)
    up_parts = across(up_parts)
    (up_block,) = kernel(
        turn_up, [((NZ, COLS, 640), bf16)], [pltpu.VMEM((2, NQ * ROWS, 256), bf16)]
    )(*up_parts)
    up_in = along_z(up_block)
    parts = kernel(split_gate, [((NZ, PART, 128), bf16)] * NQ)(block_in)
    parts = across(parts)
    final_gate, scale_gate, low, norm = kernel(
        last_gate,
        [((COLS, D_MODEL), bf16), ((1, COLS), f32), ((RANK, D_MODEL), bf16), ((NZ, NQ, 128), f32)],
        [
            pltpu.VMEM((2, NQ * ROWS, 256), bf16),
            pltpu.VMEM((2, NQ * ROWS, 128), bf16),
            pltpu.VMEM((COLS, D_MODEL), f32),
        ],
    )(*parts, mix)
    mine = norm.reshape(NZ * NQ, 128)[:, :80].astype(bf16)
    other = lax.ppermute(mine, "cols", [(0, 1), (1, 0)])
    first = lax.axis_index("cols") == 0
    serve_norm = jnp.stack(
        [jnp.where(first, mine, other), jnp.where(first, other, mine)], axis=1
    ).reshape(D_MODEL)
    final_up, scale_up = kernel(
        last_up, [((COLS, D_MODEL), bf16), ((1, COLS), f32)], [pltpu.VMEM((COLS, D_MODEL), f32)]
    )(up_in, high, low)
    return (final_gate.T, final_up.T, scale_gate[0], scale_up[0], serve_norm)


def solution(mesh):
    in_specs = (
        P(("unit", "zero"), "cols"),
        P(("unit", "zero"), None),
        P("unit", "cols"),
        P(("unit", "zero"), "cols"),
        P(("unit", "zero"), None),
        P("unit", "cols"),
        P(("unit", "zero", "cols")),
        P(("unit", "zero", "cols")),
    )
    out_specs = (
        P("unit", ("cols", "zero")),
        P("unit", ("cols", "zero")),
        P(("unit", "cols", "zero")),
        P(("unit", "cols", "zero")),
        P("unit"),
    )
    return jax.shard_map(local, mesh=mesh, in_specs=in_specs, out_specs=out_specs, check_vma=False)
```

```python
import jax
import jax.numpy as jnp
from jax import lax
from jax.experimental import pallas as pl
from jax.experimental.pallas import tpu as pltpu
from jax.sharding import PartitionSpec as P


D_MODEL = 5120
MIX = 0.5
NZ = 8
NQ = 4
ROWS = 160
COLS = 216
RANK = 32
SPAN = NQ * COLS
TILES = 7
EXTRA = 48
BLOCK = TILES * ROWS + EXTRA
PART = 2 * ROWS + EXTRA
LAST = 51

SHIFTS = (4, 3, 5, 2, 6, 1, 7)
bf16, f32 = jnp.bfloat16, jnp.float32


def lanes(shape):
    return lax.broadcasted_iota(jnp.int32, shape, len(shape) - 1)


def rows(shape):
    return lax.broadcasted_iota(jnp.int32, shape, len(shape) - 2)


def place_t(low_t, period, first):
    shape = (RANK, 128)
    hit = (lanes(shape) >= first) & ((lanes(shape) - first) % period == rows(shape))
    return lax.dot_general(
        low_t, hit.astype(bf16), (((0,), (0,)), ((), ())), preferred_element_type=f32
    )


def pack_gate(weight, low_gate, low_up, train, step, *outs):
    wide = (ROWS, 128)
    low_g = place_t(low_gate[...], 128, 96)
    low_u = place_t(low_up[...], 32, 0)
    group = lanes((40, 128)) // 32
    packed = jnp.zeros((40, 128), f32)
    for g in range(4):
        packed = jnp.where(group == g, low_u[40 * g : 40 * g + 40], packed)
    norm = jnp.concatenate([train[...] + step[...], jnp.zeros((1, 48), f32)], axis=1)
    norm = jnp.broadcast_to(norm, (8, 128))
    extra = jnp.concatenate([packed, norm], axis=0).astype(bf16)
    here = lax.axis_index("zero") // NQ
    for k in range(NZ):
        start = SPAN * ((here + k) % NZ)
        tile = jnp.minimum(start // 128, LAST - 5)
        x = weight[:, pl.ds(pl.multiple_of(tile * 128, 128), 1024)].astype(f32)
        x = pltpu.roll(x, (1024 - (start - 128 * tile)) % 1024, 1)
        for j in range(TILES):
            y = x[:, 128 * j : 128 * j + 128]
            if j == TILES - 1:
                y = jnp.where(lanes(wide) < 96, y, low_g)
            outs[k][ROWS * j : ROWS * j + ROWS, :] = y.astype(bf16)
        outs[k][ROWS * TILES : BLOCK, :] = extra


def window(x, off):
    return pltpu.roll(x, (384 - off) % 384, 1)[:, :256]


def pack_up(weight, high_gate, high_up, *outs):
    parts, mix, high = outs[:NQ], outs[NQ], outs[NQ + 1]
    place = lax.axis_index("zero")
    q = place % NQ
    for p in range(NQ):
        for z in range(NZ):
            start = COLS * (z * NQ + jnp.bitwise_xor(q, p))
            tile = jnp.minimum(start // 128, LAST)
            x = weight[:, pl.ds(pl.multiple_of(tile * 128, 128), 384)].astype(f32)
            x = window(x, start - 128 * tile).astype(bf16)
            parts[p][z, 0:ROWS, :] = x[:, :128]
            parts[p][z, ROWS : 2 * ROWS, :] = x[:, 128:]
    start = COLS * place
    tile = jnp.minimum(start // 128, LAST)
    at = pl.multiple_of(tile * 128, 128)

    def own(ref):
        x = pltpu.roll(ref[:, pl.ds(at, 384)].astype(f32), (384 - (start - 128 * tile)) % 384, 1)
        return x[:, :256].astype(bf16)

    def turned(h, first, width):
        shape = (RANK, width)
        hit = jnp.where(lanes(shape) == rows(shape) + first, MIX, 0.0).astype(bf16)
        return lax.dot_general(h, hit, (((0,), (0,)), ((), ())), preferred_element_type=f32)

    eye = (lanes((256, 256)) == rows((256, 256))) & (rows((256, 256)) < COLS)
    mix[...] = (eye.astype(f32) + turned(own(high_gate), COLS, 256)).astype(bf16)
    high[...] = turned(own(high_up), 0, 128).astype(bf16)


def turn_up(*refs):
    parts, outs, x = refs[:NQ], refs[NQ : NQ + NZ], refs[NQ + NZ]
    place = lax.axis_index("zero")
    q, here = place % NQ, place // NQ
    eye = (lanes((COLS, 256)) == rows((COLS, 256))).astype(bf16)
    for k in range(NZ):
        z = (here + k) % NZ
        for p in range(NQ):
            at = pl.multiple_of(jnp.bitwise_xor(q, p) * ROWS, ROWS)
            x[k % 2, pl.ds(at, ROWS), 0:128] = parts[p][z, 0:ROWS, :]
            x[k % 2, pl.ds(at, ROWS), 128:256] = parts[p][z, ROWS : 2 * ROWS, :]
        outs[k][...] = lax.dot_general(
            eye, x[k % 2], (((1,), (1,)), ((), ())), preferred_element_type=f32
        ).astype(bf16)


def split_gate(*refs):
    blocks, parts = refs[:NZ], refs[NZ:]
    place = lax.axis_index("zero")
    q, here = place % NQ, place // NQ
    wide = (ROWS, 128)
    for k, block in enumerate(blocks):
        z = (here + NZ - k) % NZ
        low = pltpu.roll(block[ROWS * 6 : ROWS * 7, :].astype(f32), 120, 1)
        for p in range(NQ):
            start = COLS * jnp.bitwise_xor(q, p)
            tile = jnp.minimum(start // 128, TILES - 3)
            x = jnp.concatenate(
                [
                    block[pl.ds(pl.multiple_of((tile + n) * ROWS, ROWS), ROWS), :].astype(f32)
                    for n in range(3)
                ],
                axis=1,
            )
            x = window(x, start - 128 * tile)
            last = jnp.where(lanes(wide) < 88, x[:, 128:], jnp.where(lanes(wide) < 120, low, 0.0))
            parts[p][z, 0:ROWS, :] = x[:, :128].astype(bf16)
            parts[p][z, ROWS : 2 * ROWS, :] = last.astype(bf16)
            parts[p][z, 2 * ROWS : PART, :] = block[ROWS * TILES : BLOCK, :]


def scales(total):
    column = jnp.sum(total, axis=1, keepdims=True) / D_MODEL
    padded = jnp.concatenate([total, jnp.zeros((256 - COLS, 128), f32)], axis=0)
    row = jnp.sum(jnp.transpose(padded), axis=0, keepdims=True) / D_MODEL
    return column, row[:, :COLS]


def magnitudes(r):
    a = jnp.abs(r)
    return sum(a[:, 128 * k : 128 * k + 128] for k in range(5))


def last_gate(*refs):
    parts, mix = refs[:NQ], refs[NQ]
    out, scale, low, norm = refs[NQ + 1 : NQ + 5]
    x, lows, sums = refs[NQ + 5 :]
    q = lax.axis_index("zero") % NQ
    total = jnp.zeros((COLS, 128), f32)
    m = mix[0:COLS, :]
    pick = (lanes((RANK, 128)) == rows((RANK, 128))).astype(bf16)
    for z in range(NZ):
        for p in range(NQ):
            at = pl.multiple_of(jnp.bitwise_xor(q, p) * ROWS, ROWS)
            x[z % 2, pl.ds(at, ROWS), 0:128] = parts[p][z, 0:ROWS, :]
            x[z % 2, pl.ds(at, ROWS), 128:256] = parts[p][z, ROWS : 2 * ROWS, :]
            extra = parts[p][z, 2 * ROWS : PART, :].astype(f32)
            wide = jnp.concatenate(
                [pltpu.roll(extra[0:40], (128 - 32 * g) % 128, 1) for g in range(4)], axis=0
            )
            lows[z % 2, pl.ds(at, ROWS), :] = wide.astype(bf16)
            norm[z, pl.ds(jnp.bitwise_xor(q, p), 1), :] = extra[40:41]
        r = lax.dot_general(m, x[z % 2], (((1,), (1,)), ((), ())), preferred_element_type=f32)
        sums[:, 640 * z : 640 * z + 640] = r
        total = total + magnitudes(r)
        low[:, 640 * z : 640 * z + 640] = lax.dot_general(
            pick, lows[z % 2], (((1,), (1,)), ((), ())), preferred_element_type=f32
        ).astype(bf16)
    column, row = scales(total)
    scale[...] = row
    out[...] = (sums[...] * (1.0 / column)).astype(bf16)


def last_up(*refs):
    blocks, high, low = refs[:NZ], refs[NZ], refs[NZ + 1]
    out, scale, sums = refs[NZ + 2 :]
    here = lax.axis_index("zero") // NQ
    total = jnp.zeros((COLS, 128), f32)
    h = high[0:COLS, 0:RANK]
    for k in range(NZ):
        at = pl.multiple_of((here + NZ - k) % NZ * 640, 640)
        r = blocks[k][...].astype(f32) + jnp.dot(
            h, low[:, pl.ds(at, 640)], preferred_element_type=f32
        )
        sums[:, pl.ds(at, 640)] = r
        total = total + magnitudes(r)
    column, row = scales(total)
    scale[...] = row
    out[...] = (sums[...] * (1.0 / column)).astype(bf16)


def kernel(body, outs, scratch=()):
    return pl.pallas_call(
        body,
        out_shape=[jax.ShapeDtypeStruct(*o) for o in outs],
        scratch_shapes=list(scratch),
        compiler_params=pltpu.CompilerParams(vmem_limit_bytes=48 * 2**20),
    )


def along_z(blocks):
    moved = list(blocks)
    for k in SHIFTS:
        pairs = [(z * NQ + q, (z + k) % NZ * NQ + q) for z in range(NZ) for q in range(NQ)]
        moved[k] = lax.ppermute(blocks[k], "zero", pairs)
    return moved


def across(parts):
    moved = [
        lax.ppermute(part, "zero", [(s, s ^ p) for s in range(NZ * NQ)])
        for p, part in enumerate(parts)
        if p
    ]
    return [parts[0], *moved]


def local(weight_gate, low_gate, high_gate, weight_up, low_up, high_up, norm_train, norm_step):
    blocks = kernel(pack_gate, [((BLOCK, 128), bf16)] * NZ)(
        weight_gate, low_gate.T, low_up.T, norm_train[None], norm_step[None]
    )
    blocks_in = along_z(blocks)
    *up_parts, mix, high = kernel(
        pack_up, [((NZ, 2 * ROWS, 128), bf16)] * NQ + [((256, 256), bf16), ((256, 128), bf16)]
    )(weight_up, high_gate, high_up)
    up_parts = across(up_parts)
    up_blocks = kernel(
        turn_up, [((COLS, 640), bf16)] * NZ, [pltpu.VMEM((2, NQ * ROWS, 256), bf16)]
    )(*up_parts)
    up_in = along_z(up_blocks)
    parts = kernel(split_gate, [((NZ, PART, 128), bf16)] * NQ)(*blocks_in)
    parts = across(parts)
    final_gate, scale_gate, low, norm = kernel(
        last_gate,
        [((COLS, D_MODEL), bf16), ((1, COLS), f32), ((RANK, D_MODEL), bf16), ((NZ, NQ, 128), f32)],
        [
            pltpu.VMEM((2, NQ * ROWS, 256), bf16),
            pltpu.VMEM((2, NQ * ROWS, 128), bf16),
            pltpu.VMEM((COLS, D_MODEL), f32),
        ],
    )(*parts, mix)
    mine = norm.reshape(NZ * NQ, 128)[:, :80].astype(bf16)
    other = lax.ppermute(mine, "cols", [(0, 1), (1, 0)])
    first = lax.axis_index("cols") == 0
    serve_norm = jnp.stack(
        [jnp.where(first, mine, other), jnp.where(first, other, mine)], axis=1
    ).reshape(D_MODEL)
    final_up, scale_up = kernel(
        last_up, [((COLS, D_MODEL), bf16), ((1, COLS), f32)], [pltpu.VMEM((COLS, D_MODEL), f32)]
    )(*up_in, high, low)
    return (final_gate.T, final_up.T, scale_gate[0], scale_up[0], serve_norm)


def solution(mesh):
    in_specs = (
        P(("unit", "zero"), "cols"),
        P(("unit", "zero"), None),
        P("unit", "cols"),
        P(("unit", "zero"), "cols"),
        P(("unit", "zero"), None),
        P("unit", "cols"),
        P(("unit", "zero", "cols")),
        P(("unit", "zero", "cols")),
    )
    out_specs = (
        P("unit", ("cols", "zero")),
        P("unit", ("cols", "zero")),
        P(("unit", "cols", "zero")),
        P(("unit", "cols", "zero")),
        P("unit"),
    )
    return jax.shard_map(local, mesh=mesh, in_specs=in_specs, out_specs=out_specs, check_vma=False)
```

```python
import jax
import jax.numpy as jnp
from jax import lax
from jax.experimental import pallas as pl
from jax.experimental.pallas import tpu as pltpu
from jax.sharding import PartitionSpec as P


D_MODEL = 5120
MIX = 0.5
NZ = 8
NQ = 4
ROWS = 160
COLS = 216
RANK = 32
SPAN = NQ * COLS
TILES = 7
EXTRA = 48
BLOCK = TILES * ROWS + EXTRA
PART = 2 * ROWS + EXTRA
LAST = 51

FIRST = (4,)
EARLY = (1, 7)
LATE = (2, 6, 3, 5)
UP = (4, 3, 5, 2, 6, 1, 7)
NEAR = (0, 1, 7, 2, 6)
FAR = (4, 3, 5)
ORDER = NEAR + FAR
bf16, f32 = jnp.bfloat16, jnp.float32


def lanes(shape):
    return lax.broadcasted_iota(jnp.int32, shape, len(shape) - 1)


def rows(shape):
    return lax.broadcasted_iota(jnp.int32, shape, len(shape) - 2)


def place_t(low_t, period, first):
    shape = (RANK, 128)
    hit = (lanes(shape) >= first) & ((lanes(shape) - first) % period == rows(shape))
    return lax.dot_general(
        low_t, hit.astype(bf16), (((0,), (0,)), ((), ())), preferred_element_type=f32
    )


def window_of(shift):
    start = SPAN * ((lax.axis_index("zero") // NQ + shift) % NZ)
    tile = jnp.minimum(start // 128, LAST - 5)
    return pl.multiple_of(tile * 128, 128), start - 128 * tile


def fetch(weight, windows, sem, shifts):
    copies = []
    for i, k in enumerate(shifts):
        at, _ = window_of(k)
        copies.append(
            pltpu.make_async_copy(weight.at[:, pl.ds(at, 1024)], windows.at[i], sem.at[i])
        )
        copies[i].start()
    return copies


def pack_block(x, shift, low, extra, out):
    _, off = window_of(shift)
    x = pltpu.roll(x.astype(f32), (1024 - off) % 1024, 1)
    for j in range(TILES):
        y = x[:, 128 * j : 128 * j + 128]
        if j == TILES - 1:
            y = jnp.where(lanes((ROWS, 128)) < 96, y, low)
        out[ROWS * j : ROWS * j + ROWS, :] = y.astype(bf16)
    out[ROWS * TILES : BLOCK, :] = extra


def pack_first(weight, low_gate, low_up, train, step, out, tail, windows, lows, norms, sem, small):
    copies = fetch(weight, windows, sem, FIRST)
    others = [
        pltpu.make_async_copy(source, target, small.at[i])
        for i, (source, target) in enumerate(
            ((low_gate, lows.at[0]), (low_up, lows.at[1]), (train, norms.at[0]), (step, norms.at[1]))
        )
    ]
    for copy in others:
        copy.start()
    for copy in others:
        copy.wait()
    low_g = place_t(lows[0], 128, 96)
    low_u = place_t(lows[1], 32, 0)
    group = lanes((40, 128)) // 32
    packed = jnp.zeros((40, 128), f32)
    for g in range(4):
        packed = jnp.where(group == g, low_u[40 * g : 40 * g + 40], packed)
    norm = jnp.concatenate([norms[0] + norms[1], jnp.zeros((1, 48), f32)], axis=1)
    norm = jnp.broadcast_to(norm, (8, 128))
    extra = jnp.concatenate([packed, norm], axis=0).astype(bf16)
    tail[0:ROWS, :] = low_g.astype(bf16)
    tail[ROWS : ROWS + EXTRA, :] = extra
    copies[0].wait()
    pack_block(windows[0], FIRST[0], low_g, extra, out)


def pack_rest(weight, tail, *refs):
    shifts = (*EARLY, *LATE, 0)
    outs, windows, sem = refs[: len(shifts)], refs[-2], refs[-1]
    copies = fetch(weight, windows, sem, shifts)
    low = tail[0:ROWS, :].astype(f32)
    extra = tail[ROWS : ROWS + EXTRA, :]
    for i, k in enumerate(shifts):
        copies[i].wait()
        pack_block(windows[i], k, low, extra, outs[i])


def window(x, off):
    return pltpu.roll(x, (384 - off) % 384, 1)[:, :256]


def pack_up(weight, *parts):
    q = lax.axis_index("zero") % NQ
    for p in range(NQ):
        for z in range(NZ):
            start = COLS * (z * NQ + jnp.bitwise_xor(q, p))
            tile = jnp.minimum(start // 128, LAST)
            x = weight[:, pl.ds(pl.multiple_of(tile * 128, 128), 384)].astype(f32)
            x = window(x, start - 128 * tile)
            parts[p][z, 0:ROWS, :] = x[:, :128].astype(bf16)
            parts[p][z, ROWS : 2 * ROWS, :] = x[:, 128:].astype(bf16)


def turn_high(high_gate, high_up, mix, high, highs, sem):
    start = COLS * lax.axis_index("zero")
    tile = jnp.minimum(start // 128, LAST)
    own = pl.ds(pl.multiple_of(tile * 128, 128), 384)
    copies = [
        pltpu.make_async_copy(source.at[:, own], highs.at[i], sem.at[i])
        for i, source in enumerate((high_gate, high_up))
    ]
    for copy in copies:
        copy.start()
    for copy in copies:
        copy.wait()

    def own_high(i):
        x = pltpu.roll(highs[i].astype(f32), (384 - (start - 128 * tile)) % 384, 1)
        return x[:, :256].astype(bf16)

    def turned(h, first, width):
        shape = (RANK, width)
        hit = jnp.where(lanes(shape) == rows(shape) + first, MIX, 0.0).astype(bf16)
        return lax.dot_general(h, hit, (((0,), (0,)), ((), ())), preferred_element_type=f32)

    eye = (lanes((256, 256)) == rows((256, 256))) & (rows((256, 256)) < COLS)
    mix[...] = (eye.astype(f32) + turned(own_high(0), COLS, 256)).astype(bf16)
    high[...] = turned(own_high(1), 0, 128).astype(bf16)


def turn_up(*refs):
    parts, outs, x = refs[:NQ], refs[NQ : NQ + NZ], refs[NQ + NZ]
    place = lax.axis_index("zero")
    q, here = place % NQ, place // NQ
    eye = (lanes((COLS, 256)) == rows((COLS, 256))).astype(bf16)
    for k in (*UP, 0):
        z = (here + k) % NZ
        for p in range(NQ):
            at = pl.multiple_of(jnp.bitwise_xor(q, p) * ROWS, ROWS)
            x[k % 2, pl.ds(at, ROWS), 0:128] = parts[p][z, 0:ROWS, :]
            x[k % 2, pl.ds(at, ROWS), 128:256] = parts[p][z, ROWS : 2 * ROWS, :]
        outs[k][...] = lax.dot_general(
            eye, x[k % 2], (((1,), (1,)), ((), ())), preferred_element_type=f32
        ).astype(bf16)


def split_gate(*refs):
    count = len(refs) - NQ
    blocks, parts = refs[:count], refs[count:]
    q = lax.axis_index("zero") % NQ
    wide = (ROWS, 128)
    for i, block in enumerate(blocks):
        low = pltpu.roll(block[ROWS * 6 : ROWS * 7, :].astype(f32), 120, 1)
        for p in range(NQ):
            start = COLS * jnp.bitwise_xor(q, p)
            tile = jnp.minimum(start // 128, TILES - 3)
            x = jnp.concatenate(
                [
                    block[pl.ds(pl.multiple_of((tile + n) * ROWS, ROWS), ROWS), :].astype(f32)
                    for n in range(3)
                ],
                axis=1,
            )
            x = window(x, start - 128 * tile)
            last = jnp.where(lanes(wide) < 88, x[:, 128:], jnp.where(lanes(wide) < 120, low, 0.0))
            parts[p][i, 0:ROWS, :] = x[:, :128].astype(bf16)
            parts[p][i, ROWS : 2 * ROWS, :] = last.astype(bf16)
            parts[p][i, 2 * ROWS : PART, :] = block[ROWS * TILES : BLOCK, :]


def scales(total):
    column = jnp.sum(total, axis=1, keepdims=True) / D_MODEL
    padded = jnp.concatenate([total, jnp.zeros((256 - COLS, 128), f32)], axis=0)
    row = jnp.sum(jnp.transpose(padded), axis=0, keepdims=True) / D_MODEL
    return column, row[:, :COLS]


def magnitudes(r):
    a = jnp.abs(r)
    return sum(a[:, 128 * k : 128 * k + 128] for k in range(5))


def norm_rows(*refs):
    place = lax.axis_index("zero")
    q, here = place % NQ, place // NQ
    for i, k in enumerate(ORDER):
        z = (here + NZ - k) % NZ
        half, j = (0, i) if i < len(NEAR) else (1, i - len(NEAR))
        for p in range(NQ):
            extra = refs[NQ * half + p][j, 2 * ROWS : PART, :].astype(f32)
            refs[2 * NQ][pl.ds(NQ * z + jnp.bitwise_xor(q, p), 1), :] = extra[40:41]


def norm_join(mine, other, out):
    first = 80 * lax.axis_index("cols")
    total = jnp.zeros((40, 128), f32)
    for source, start in ((mine, first), (other, 80 - first)):
        values = source[...].astype(bf16)
        for j in range(5):
            for m in range(NQ):
                if 160 * m >= 128 * (j + 1) or 160 * (m + 1) <= 128 * j:
                    continue
                shape = (40, NZ * NQ)
                at = rows(shape)
                row = (at % 5 == j) & (lanes(shape) == at // 5 * NQ + m)
                picked = jnp.dot(row.astype(bf16), values, preferred_element_type=f32)
                shape = (128, 128)
                lane = (rows(shape) < 80) & (rows(shape) + start + 160 * m == lanes(shape) + 128 * j)
                total = total + jnp.dot(
                    picked.astype(bf16), lane.astype(bf16), preferred_element_type=f32
                )
    out[...] = total.astype(bf16)


def last_gate(*refs):
    near, far, (mix, out, scale, low) = refs[:NQ], refs[NQ : 2 * NQ], refs[2 * NQ : 2 * NQ + 4]
    x, lows, sums = refs[2 * NQ + 4 :]
    place = lax.axis_index("zero")
    q, here = place % NQ, place // NQ
    total = jnp.zeros((COLS, 128), f32)
    m = mix[0:COLS, :]
    pick = (lanes((RANK, 128)) == rows((RANK, 128))).astype(bf16)
    turned = (((1,), (1,)), ((), ()))
    for i, k in enumerate(ORDER):
        parts, j = (near, i) if i < len(NEAR) else (far, i - len(NEAR))
        for p in range(NQ):
            at = pl.multiple_of(jnp.bitwise_xor(q, p) * ROWS, ROWS)
            x[i % 2, pl.ds(at, ROWS), 0:128] = parts[p][j, 0:ROWS, :]
            x[i % 2, pl.ds(at, ROWS), 128:256] = parts[p][j, ROWS : 2 * ROWS, :]
            extra = parts[p][j, 2 * ROWS : PART, :].astype(f32)[0:40]
            wide = jnp.concatenate(
                [pltpu.roll(extra, (128 - 32 * g) % 128, 1) for g in range(4)], axis=0
            )
            lows[i % 2, pl.ds(at, ROWS), :] = wide.astype(bf16)
        at = pl.multiple_of((here + NZ - k) % NZ * 640, 640)
        r = lax.dot_general(m, x[i % 2], turned, preferred_element_type=f32)
        sums[:, pl.ds(at, 640)] = r
        total = total + magnitudes(r)
        low[:, pl.ds(at, 640)] = lax.dot_general(
            pick, lows[i % 2], turned, preferred_element_type=f32
        ).astype(bf16)
    column, row = scales(total)
    scale[...] = row
    out[...] = (sums[...] * (1.0 / column)).astype(bf16)


def last_up(*refs):
    blocks, high, low = refs[:NZ], refs[NZ], refs[NZ + 1]
    out, scale, sums = refs[NZ + 3 :]
    here = lax.axis_index("zero") // NQ
    total = jnp.zeros((COLS, 128), f32)
    h = high[0:COLS, 0:RANK]
    for k in range(NZ):
        at = pl.multiple_of((here + NZ - k) % NZ * 640, 640)
        r = blocks[k][...].astype(f32) + jnp.dot(
            h, low[:, pl.ds(at, 640)], preferred_element_type=f32
        )
        sums[:, pl.ds(at, 640)] = r
        total = total + magnitudes(r)
    column, row = scales(total)
    scale[...] = row
    out[...] = (sums[...] * (1.0 / column)).astype(bf16)


HBM, VMEM = pl.BlockSpec(memory_space=pltpu.HBM), pl.BlockSpec(memory_space=pltpu.VMEM)


def kernel(body, outs, scratch=(), ins=None, places=None):
    specs = {} if ins is None else {"in_specs": ins}
    if places is not None:
        specs["out_specs"] = places
    return pl.pallas_call(
        body,
        out_shape=[jax.ShapeDtypeStruct(*o) for o in outs],
        scratch_shapes=list(scratch),
        compiler_params=pltpu.CompilerParams(vmem_limit_bytes=24 * 2**20),
        **specs,
    )


def hbm(x):
    return pltpu.with_memory_space_constraint(x, pltpu.HBM)


def along_z(block, shift):
    pairs = [(z * NQ + q, (z + shift) % NZ * NQ + q) for z in range(NZ) for q in range(NQ)]
    return lax.ppermute(block, "zero", pairs)


def across(parts):
    moved = [
        lax.ppermute(part, "zero", [(s, s ^ p) for s in range(NZ * NQ)])
        for p, part in enumerate(parts)
        if p
    ]
    return [parts[0], *moved]


def local(weight_gate, low_gate, high_gate, weight_up, low_up, high_up, norm_train, norm_step):
    dma = pltpu.SemaphoreType.DMA
    inward = {}
    first, tail = kernel(
        pack_first,
        [((BLOCK, 128), bf16), ((ROWS + EXTRA, 128), bf16)],
        [
            pltpu.VMEM((1, ROWS, 1024), bf16),
            pltpu.VMEM((2, RANK, ROWS), bf16),
            pltpu.VMEM((2, 1, 80), f32),
            dma((1,)),
            dma((4,)),
        ],
        [HBM] * 5,
    )(*map(hbm, (weight_gate, low_gate.T, low_up.T, norm_train[None], norm_step[None])))
    inward[FIRST[0]] = along_z(first, FIRST[0])
    shifts = (*EARLY, *LATE, 0)
    blocks = kernel(
        pack_rest,
        [((BLOCK, 128), bf16)] * len(shifts),
        [pltpu.VMEM((len(shifts), ROWS, 1024), bf16), dma((len(shifts),))],
        [HBM, VMEM],
    )(hbm(weight_gate), tail)
    for k, block in zip(shifts, blocks):
        inward[k] = along_z(block, k) if k else block
    up_parts = kernel(pack_up, [((NZ, 2 * ROWS, 128), bf16)] * NQ)(weight_up)
    up_parts = across(up_parts)
    up_blocks = kernel(
        turn_up, [((COLS, 640), bf16)] * NZ, [pltpu.VMEM((2, NQ * ROWS, 256), bf16)]
    )(*up_parts)
    up_in = list(up_blocks)
    for k in UP:
        up_in[k] = along_z(up_blocks[k], k)
    halves = []
    for shifts in (NEAR, FAR):
        parts = kernel(
            split_gate, [((len(shifts), PART, 128), bf16)] * NQ
        )(*[inward[k] for k in shifts])
        halves.append(across(parts))
    mix, high = kernel(
        turn_high,
        [((256, 256), bf16), ((256, 128), bf16)],
        [pltpu.VMEM((2, RANK, 384), bf16), dma((2,))],
        [HBM, HBM],
    )(hbm(high_gate), hbm(high_up))
    (norm,) = kernel(norm_rows, [((NZ * NQ, 128), f32)])(*halves[0], *halves[1])
    final_gate, scale_gate, low = kernel(
        last_gate,
        [((COLS, D_MODEL), bf16), ((1, COLS), f32), ((RANK, D_MODEL), bf16)],
        [
            pltpu.VMEM((2, NQ * ROWS, 256), bf16),
            pltpu.VMEM((2, NQ * ROWS, 128), bf16),
            pltpu.VMEM((COLS, D_MODEL), f32),
        ],
    )(*halves[0], *halves[1], mix)
    other = lax.ppermute(norm, "cols", [(0, 1), (1, 0)])
    (serve_norm,) = kernel(norm_join, [((40, 128), bf16)])(norm, other)
    final_up, scale_up = kernel(
        last_up,
        [((COLS, D_MODEL), bf16), ((1, COLS), f32)],
        [pltpu.VMEM((COLS, D_MODEL), f32)],
        [VMEM] * (NZ + 2) + [HBM],
    )(*up_in, high, low, hbm(serve_norm))
    return (final_gate.T, final_up.T, scale_gate[0], scale_up[0], serve_norm.reshape(D_MODEL))


def solution(mesh):
    in_specs = (
        P(("unit", "zero"), "cols"),
        P(("unit", "zero"), None),
        P("unit", "cols"),
        P(("unit", "zero"), "cols"),
        P(("unit", "zero"), None),
        P("unit", "cols"),
        P(("unit", "zero", "cols")),
        P(("unit", "zero", "cols")),
    )
    out_specs = (
        P("unit", ("cols", "zero")),
        P("unit", ("cols", "zero")),
        P(("unit", "cols", "zero")),
        P(("unit", "cols", "zero")),
        P("unit"),
    )
    return jax.shard_map(local, mesh=mesh, in_specs=in_specs, out_specs=out_specs, check_vma=False)
```

```python
import jax
import jax.numpy as jnp
from jax import lax
from jax.experimental import pallas as pl
from jax.experimental.pallas import tpu as pltpu
from jax.sharding import PartitionSpec as P


D_MODEL = 5120
MIX = 0.5
NZ = 8
NQ = 4
ROWS = 160
COLS = 216
RANK = 32
SPAN = NQ * COLS
TILES = 7
BLOCK = TILES * ROWS + 8
PART = 2 * ROWS + 16
LAST = 51

FIRST = (4,)
EARLY = (1, 7)
LATE = (2, 6, 3, 5)
UP = (4, 3, 5, 2, 6, 1, 7)
NEAR = (0, 1, 7, 2, 6)
FAR = (4, 3, 5)
ORDER = NEAR + FAR
bf16, f32 = jnp.bfloat16, jnp.float32


def lanes(shape):
    return lax.broadcasted_iota(jnp.int32, shape, len(shape) - 1)


def rows(shape):
    return lax.broadcasted_iota(jnp.int32, shape, len(shape) - 2)


def window_of(shift):
    start = SPAN * ((lax.axis_index("zero") // NQ + shift) % NZ)
    tile = jnp.minimum(start // 128, LAST - 5)
    return pl.multiple_of(tile * 128, 128), start - 128 * tile


def fetch(weight, windows, sem, shifts):
    copies = []
    for i, k in enumerate(shifts):
        at, _ = window_of(k)
        copies.append(
            pltpu.make_async_copy(weight.at[:, pl.ds(at, 1024)], windows.at[i], sem.at[i])
        )
        copies[i].start()
    return copies


def pack_block(x, shift, low, extra, out):
    _, off = window_of(shift)
    x = pltpu.roll(x.astype(f32), (1024 - off) % 1024, 1)
    for j in range(TILES):
        y = x[:, 128 * j : 128 * j + 128]
        if j == TILES - 1:
            y = jnp.where(lanes((ROWS, 128)) < 96, y, low)
        out[ROWS * j : ROWS * j + ROWS, :] = y.astype(bf16)
    out[ROWS * TILES : BLOCK, :] = extra


def pack_first(weight, low_gate, low_up, train, step, out, tail, windows, lows, norms, sem, small):
    copies = fetch(weight, windows, sem, FIRST)
    others = [
        pltpu.make_async_copy(source, target, small.at[i])
        for i, (source, target) in enumerate(
            ((low_gate, lows.at[0]), (low_up, lows.at[1]), (train, norms.at[0]), (step, norms.at[1]))
        )
    ]
    for copy in others:
        copy.start()
    for copy in others:
        copy.wait()
    mine = jnp.where(lax.axis_index("cols") == 0, lows[0].astype(f32), lows[1].astype(f32))
    shape = (RANK, 128)
    low = lax.dot_general(
        mine.astype(bf16),
        (lanes(shape) == rows(shape) + 96).astype(bf16),
        (((0,), (0,)), ((), ())),
        preferred_element_type=f32,
    )
    norm = jnp.concatenate([norms[0] + norms[1], jnp.zeros((1, 48), f32)], axis=1)
    extra = jnp.broadcast_to(norm, (8, 128))
    tail[0:ROWS, :] = low
    tail[ROWS : ROWS + 8, :] = extra
    copies[0].wait()
    pack_block(windows[0], FIRST[0], low, extra.astype(bf16), out)


def pack_rest(weight, tail, *refs):
    shifts = (*EARLY, *LATE, 0)
    outs, windows, sem = refs[: len(shifts)], refs[-2], refs[-1]
    copies = fetch(weight, windows, sem, shifts)
    low = tail[0:ROWS, :]
    extra = tail[ROWS : ROWS + 8, :].astype(bf16)
    for i, k in enumerate(shifts):
        copies[i].wait()
        pack_block(windows[i], k, low, extra, outs[i])


def window(x, off):
    return pltpu.roll(x, (384 - off) % 384, 1)[:, :256]


def pack_up(weight, *parts):
    q = lax.axis_index("zero") % NQ
    for p in range(NQ):
        for z in range(NZ):
            start = COLS * (z * NQ + jnp.bitwise_xor(q, p))
            tile = jnp.minimum(start // 128, LAST)
            x = weight[:, pl.ds(pl.multiple_of(tile * 128, 128), 384)].astype(f32)
            x = window(x, start - 128 * tile)
            parts[p][z, 0:ROWS, :] = x[:, :128].astype(bf16)
            parts[p][z, ROWS : 2 * ROWS, :] = x[:, 128:].astype(bf16)


def turn_high(high_gate, high_up, *refs):
    turned, highs, sem = refs[:2], refs[2], refs[3]
    start = COLS * lax.axis_index("zero")
    tile = jnp.minimum(start // 128, LAST)
    own = pl.ds(pl.multiple_of(tile * 128, 128), 384)
    copies = [
        pltpu.make_async_copy(source.at[:, own], highs.at[i], sem.at[i])
        for i, source in enumerate((high_gate, high_up))
    ]
    for copy in copies:
        copy.start()
    for copy in copies:
        copy.wait()
    shape = (RANK, 128)
    half = jnp.where(lanes(shape) == rows(shape), MIX, 0.0).astype(bf16)
    for i in range(2):
        x = pltpu.roll(highs[i].astype(f32), (384 - (start - 128 * tile)) % 384, 1)
        turned[i][...] = lax.dot_general(
            x[:, :256].astype(bf16), half, (((0,), (0,)), ((), ())), preferred_element_type=f32
        ).astype(bf16)


def turn_up(*refs):
    parts, outs, x = refs[:NQ], refs[NQ : NQ + NZ], refs[NQ + NZ]
    place = lax.axis_index("zero")
    q, here = place % NQ, place // NQ
    eye = (lanes((COLS, 256)) == rows((COLS, 256))).astype(bf16)
    for k in (*UP, 0):
        z = (here + k) % NZ
        for p in range(NQ):
            at = pl.multiple_of(jnp.bitwise_xor(q, p) * ROWS, ROWS)
            x[k % 2, pl.ds(at, ROWS), 0:128] = parts[p][z, 0:ROWS, :]
            x[k % 2, pl.ds(at, ROWS), 128:256] = parts[p][z, ROWS : 2 * ROWS, :]
        outs[k][...] = lax.dot_general(
            eye, x[k % 2], (((1,), (1,)), ((), ())), preferred_element_type=f32
        ).astype(bf16)


def split_gate(*refs):
    count = len(refs) - NQ
    blocks, parts = refs[:count], refs[count:]
    q = lax.axis_index("zero") % NQ
    wide = (ROWS, 128)
    for i, block in enumerate(blocks):
        low = pltpu.roll(block[ROWS * 6 : ROWS * 7, :].astype(f32), 120, 1)
        norm = block[ROWS * TILES : BLOCK, :].astype(f32)
        norm = jnp.concatenate([norm, norm], axis=0).astype(bf16)
        for p in range(NQ):
            start = COLS * jnp.bitwise_xor(q, p)
            tile = jnp.minimum(start // 128, TILES - 3)
            x = jnp.concatenate(
                [
                    block[pl.ds(pl.multiple_of((tile + n) * ROWS, ROWS), ROWS), :].astype(f32)
                    for n in range(3)
                ],
                axis=1,
            )
            x = window(x, start - 128 * tile)
            last = jnp.where(lanes(wide) < 88, x[:, 128:], jnp.where(lanes(wide) < 120, low, 0.0))
            parts[p][i, 0:ROWS, :] = x[:, :128].astype(bf16)
            parts[p][i, ROWS : 2 * ROWS, :] = last.astype(bf16)
            parts[p][i, 2 * ROWS : PART, :] = norm


def scales(total):
    column = jnp.sum(total, axis=1, keepdims=True) / D_MODEL
    padded = jnp.concatenate([total, jnp.zeros((256 - COLS, 128), f32)], axis=0)
    row = jnp.sum(jnp.transpose(padded), axis=0, keepdims=True) / D_MODEL
    return column, row[:, :COLS]


def magnitudes(r):
    a = jnp.abs(r)
    return sum(a[:, 128 * k : 128 * k + 128] for k in range(5))


def norm_rows(*refs):
    place = lax.axis_index("zero")
    q, here = place % NQ, place // NQ
    for i, k in enumerate(ORDER):
        z = (here + NZ - k) % NZ
        half, j = (0, i) if i < len(NEAR) else (1, i - len(NEAR))
        for p in range(NQ):
            extra = refs[NQ * half + p][j, 2 * ROWS : PART, :].astype(f32)
            refs[2 * NQ][pl.ds(NQ * z + jnp.bitwise_xor(q, p), 1), :] = extra[0:1]


def norm_join(mine, other, out):
    first = 80 * lax.axis_index("cols")
    total = jnp.zeros((40, 128), f32)
    for source, start in ((mine, first), (other, 80 - first)):
        values = source[...].astype(bf16)
        for j in range(5):
            for m in range(NQ):
                if 160 * m >= 128 * (j + 1) or 160 * (m + 1) <= 128 * j:
                    continue
                shape = (40, NZ * NQ)
                at = rows(shape)
                row = (at % 5 == j) & (lanes(shape) == at // 5 * NQ + m)
                picked = jnp.dot(row.astype(bf16), values, preferred_element_type=f32)
                shape = (128, 128)
                lane = (rows(shape) < 80) & (rows(shape) + start + 160 * m == lanes(shape) + 128 * j)
                total = total + jnp.dot(
                    picked.astype(bf16), lane.astype(bf16), preferred_element_type=f32
                )
    out[...] = total.astype(bf16)


def block_of(i, halves):
    return (halves[:NQ], i) if i < len(NEAR) else (halves[NQ:], i - len(NEAR))


def low_rows(*refs):
    halves, out, x = refs[: 2 * NQ], refs[2 * NQ], refs[2 * NQ + 1]
    place = lax.axis_index("zero")
    q, here = place % NQ, place // NQ
    pick = (lanes((RANK, 128)) == rows((RANK, 128)) + (COLS - 128)).astype(bf16)
    for i, k in enumerate(ORDER):
        parts, j = block_of(i, halves)
        for p in range(NQ):
            at = pl.multiple_of(jnp.bitwise_xor(q, p) * ROWS, ROWS)
            x[i % 2, pl.ds(at, ROWS), :] = parts[p][j, ROWS : 2 * ROWS, :]
        at = pl.multiple_of((here + NZ - k) % NZ * 640, 640)
        out[:, pl.ds(at, 640)] = lax.dot_general(
            pick, x[i % 2], (((1,), (1,)), ((), ())), preferred_element_type=f32
        ).astype(bf16)


def last_gate(*refs):
    halves, (high, mine, other, out, scale, low_up) = refs[: 2 * NQ], refs[2 * NQ : 2 * NQ + 6]
    x, sums = refs[2 * NQ + 6 :]
    place = lax.axis_index("zero")
    q, here = place % NQ, place // NQ
    has_gate = lax.axis_index("cols") == 0
    total = jnp.zeros((COLS, 128), f32)
    eye = (lanes((COLS, 256)) == rows((COLS, 256))).astype(bf16)
    h = high[0:COLS, 0:RANK]
    for i, k in enumerate(ORDER):
        parts, j = block_of(i, halves)
        for p in range(NQ):
            at = pl.multiple_of(jnp.bitwise_xor(q, p) * ROWS, ROWS)
            x[i % 2, pl.ds(at, ROWS), 0:128] = parts[p][j, 0:ROWS, :]
            x[i % 2, pl.ds(at, ROWS), 128:256] = parts[p][j, ROWS : 2 * ROWS, :]
        at = pl.multiple_of((here + NZ - k) % NZ * 640, 640)
        a, b = mine[:, pl.ds(at, 640)].astype(f32), other[:, pl.ds(at, 640)].astype(f32)
        low = jnp.where(has_gate, a, b).astype(bf16)
        low_up[:, pl.ds(at, 640)] = jnp.where(has_gate, b, a).astype(bf16)
        r = lax.dot_general(
            eye, x[i % 2], (((1,), (1,)), ((), ())), preferred_element_type=f32
        ) + jnp.dot(h, low, preferred_element_type=f32)
        sums[:, pl.ds(at, 640)] = r
        total = total + magnitudes(r)
    column, row = scales(total)
    scale[...] = row
    out[...] = (sums[...] * (1.0 / column)).astype(bf16)


def last_up(*refs):
    blocks, high, low = refs[:NZ], refs[NZ], refs[NZ + 1]
    out, scale, sums = refs[NZ + 3 :]
    here = lax.axis_index("zero") // NQ
    total = jnp.zeros((COLS, 128), f32)
    h = high[0:COLS, 0:RANK]
    for k in range(NZ):
        at = pl.multiple_of((here + NZ - k) % NZ * 640, 640)
        r = blocks[k][...].astype(f32) + jnp.dot(
            h, low[:, pl.ds(at, 640)], preferred_element_type=f32
        )
        sums[:, pl.ds(at, 640)] = r
        total = total + magnitudes(r)
    column, row = scales(total)
    scale[...] = row
    out[...] = (sums[...] * (1.0 / column)).astype(bf16)


HBM, VMEM = pl.BlockSpec(memory_space=pltpu.HBM), pl.BlockSpec(memory_space=pltpu.VMEM)


def kernel(body, outs, scratch=(), ins=None, places=None):
    specs = {} if ins is None else {"in_specs": ins}
    if places is not None:
        specs["out_specs"] = places
    return pl.pallas_call(
        body,
        out_shape=[jax.ShapeDtypeStruct(*o) for o in outs],
        scratch_shapes=list(scratch),
        compiler_params=pltpu.CompilerParams(vmem_limit_bytes=24 * 2**20),
        **specs,
    )


def hbm(x):
    return pltpu.with_memory_space_constraint(x, pltpu.HBM)


def along_z(block, shift):
    pairs = [(z * NQ + q, (z + shift) % NZ * NQ + q) for z in range(NZ) for q in range(NQ)]
    return lax.ppermute(block, "zero", pairs)


def across(parts):
    moved = [
        lax.ppermute(part, "zero", [(s, s ^ p) for s in range(NZ * NQ)])
        for p, part in enumerate(parts)
        if p
    ]
    return [parts[0], *moved]


def local(weight_gate, low_gate, high_gate, weight_up, low_up, high_up, norm_train, norm_step):
    dma = pltpu.SemaphoreType.DMA
    inward = {}
    first, tail = kernel(
        pack_first,
        [((BLOCK, 128), bf16), ((ROWS + 8, 128), f32)],
        [
            pltpu.VMEM((1, ROWS, 1024), bf16),
            pltpu.VMEM((2, RANK, ROWS), bf16),
            pltpu.VMEM((2, 1, 80), f32),
            dma((1,)),
            dma((4,)),
        ],
        [HBM] * 5,
    )(*map(hbm, (weight_gate, low_gate.T, low_up.T, norm_train[None], norm_step[None])))
    inward[FIRST[0]] = along_z(first, FIRST[0])
    shifts = (*EARLY, *LATE, 0)
    blocks = kernel(
        pack_rest,
        [((BLOCK, 128), bf16)] * len(shifts),
        [pltpu.VMEM((len(shifts), ROWS, 1024), bf16), dma((len(shifts),))],
        [HBM, VMEM],
    )(hbm(weight_gate), tail)
    for k, block in zip(shifts, blocks):
        inward[k] = along_z(block, k) if k else block
    up_parts = kernel(pack_up, [((NZ, 2 * ROWS, 128), bf16)] * NQ)(weight_up)
    up_parts = across(up_parts)
    up_blocks = kernel(
        turn_up, [((COLS, 640), bf16)] * NZ, [pltpu.VMEM((2, NQ * ROWS, 256), bf16)]
    )(*up_parts)
    up_in = list(up_blocks)
    for k in UP:
        up_in[k] = along_z(up_blocks[k], k)
    halves = []
    for shifts in (NEAR, FAR):
        parts = kernel(
            split_gate, [((len(shifts), PART, 128), bf16)] * NQ
        )(*[inward[k] for k in shifts])
        halves.append(across(parts))
    arrived = (*halves[0], *halves[1])
    (norm,) = kernel(norm_rows, [((NZ * NQ, 128), f32)])(*arrived)
    (low,) = kernel(
        low_rows, [((RANK, D_MODEL), bf16)], [pltpu.VMEM((2, NQ * ROWS, 128), bf16)]
    )(*arrived)
    other_low = lax.ppermute(low, "cols", [(0, 1), (1, 0)])
    other = lax.ppermute(norm, "cols", [(0, 1), (1, 0)])
    high_g, high_u = kernel(
        turn_high,
        [((256, 128), bf16)] * 2,
        [pltpu.VMEM((2, RANK, 384), bf16), dma((2,))],
        [HBM, HBM],
    )(hbm(high_gate), hbm(high_up))
    (serve_norm,) = kernel(norm_join, [((40, 128), bf16)])(norm, other)
    final_gate, scale_gate, low_u = kernel(
        last_gate,
        [((COLS, D_MODEL), bf16), ((1, COLS), f32), ((RANK, D_MODEL), bf16)],
        [pltpu.VMEM((2, NQ * ROWS, 256), bf16), pltpu.VMEM((COLS, D_MODEL), f32)],
    )(*arrived, high_g, low, other_low)
    final_up, scale_up = kernel(
        last_up,
        [((COLS, D_MODEL), bf16), ((1, COLS), f32)],
        [pltpu.VMEM((COLS, D_MODEL), f32)],
        [VMEM] * (NZ + 2) + [HBM],
    )(*up_in, high_u, low_u, hbm(serve_norm))
    return (final_gate.T, final_up.T, scale_gate[0], scale_up[0], serve_norm.reshape(D_MODEL))


def solution(mesh):
    in_specs = (
        P(("unit", "zero"), "cols"),
        P(("unit", "zero"), None),
        P("unit", "cols"),
        P(("unit", "zero"), "cols"),
        P(("unit", "zero"), None),
        P("unit", "cols"),
        P(("unit", "zero", "cols")),
        P(("unit", "zero", "cols")),
    )
    out_specs = (
        P("unit", ("cols", "zero")),
        P("unit", ("cols", "zero")),
        P(("unit", "cols", "zero")),
        P(("unit", "cols", "zero")),
        P("unit"),
    )
    return jax.shard_map(local, mesh=mesh, in_specs=in_specs, out_specs=out_specs, check_vma=False)
```
